32 devices in a mesh: tile: 8 (over z, x), lev: 4 (over y, core).
Axes of the slice: x: 2, y: 2, z: 4, core: 2. Of those that a mesh axis runs over, the one named last changes fastest.
Arguments:
- mixing: float32 [3, 64, 32768], P(None, 'lev', 'tile'), may hold values from 0.05 to 3
- density: float32 [64, 32768], P('lev', 'tile'), may hold values from 0.4 to 1.2
- routes: int32 [32768, 1], P('tile'), may hold values from 0 to 7; in each aligned block of 4096 rows (0 to 4095, 4096 to 8191, ...) at most 1024 rows name the same one
- beam_weight: float32 [8, 168, 64], P('tile'), may hold values from 0.001 to 0.06
- gate_adjoint: float32 [168, 65536], P('lev', 'tile'), may hold values from -6 to 6
Outputs:
- gate_values: float32 [168, 65536], P('lev', 'tile')
- increments: float32 [3, 64, 32768], P(None, 'lev', 'tile')
The draws below stay inside these ranges and needn't reach their ends.
Inputs may be any that keep to these rules, and one draw needn't show every extreme that they name: `routes`: each column names the site that observes it; the columns of one tile index send at most 1024 columns to one site, and exactly 1024 to some site.
All inputs are finite; a program needn't handle non-finite values.
Results may differ from the reference program's by a relative error of at most 0.00007.
Values sent between devices are 32-bit elements; how exact they have to be, the bound alone decides.
No kernel may reach another device: no remote copies, remote signals or barrier semaphores. Data moves between devices by JAX's collectives and lax.ppermute only.
A program may use at most 64 MiB of HBM per device.

```python
import math
import jax
import jax.numpy as jnp
import numpy as np
from jax import lax

COL_DEV = 4096
LEV = 64
GATE_COL = 168
SITES = 8
CAP = 1024
COLS = 32768
SLOTS = 65536
N_TILE = 8


def levels(stream_key, extent, shards, low, high):
    def one(axis_at, parts):
        steps = jax.random.uniform(jax.random.fold_in(jax.random.fold_in(stream_key, 6), axis_at), (parts,), jnp.float32, low / len(shards), high / len(shards))
        return jnp.repeat(jnp.exp(steps), extent[axis_at] // parts).reshape((-1,) + (1,) * (len(extent) - axis_at - 1))

    factor_of = one(*shards[0])
    for cut in shards[1:]:
        factor_of = factor_of * one(*cut)
    return factor_of


def deal_out(own_key, own, number, rows, number_of, top, most, lean):
    order = jax.random.permutation(own_key, number_of)
    crowded, ordinary = shares(number_of, rows * top, most, lean, True), shares(number_of, rows * top, most, lean, False)
    places = jnp.arange(number_of)

    def named(lengths, turn):
        used = int((lengths > 0).sum())
        fixed = max(1, used // 4)
        moved = fixed + (places - fixed + turn * (used - fixed)) % max(1, number_of - fixed)
        return jnp.zeros((number_of,), jnp.int32).at[order[jnp.where(places < fixed, places, moved)]].set(jnp.asarray(lengths, jnp.int32))

    lengths = jnp.where(number % 4 == 0, named(crowded, number // 4), named(ordinary, number - number // 4 - 1))
    mixed = jax.random.permutation(jax.random.fold_in(own, 3), number_of)
    source_of, receiver = mixed[0:number_of // 2 * 2:2], mixed[1:number_of // 2 * 2:2]
    room = jnp.minimum(lengths[source_of] - 1, most - lengths[receiver]) // 2
    room = jnp.where((source_of == order[0]) | (receiver == order[0]) | (lengths[receiver] == 0), 0, jnp.maximum(room, 0))
    moved = jax.random.randint(jax.random.fold_in(own, 4), (number_of // 2,), 0, 1 << 20) % (room + 1)
    lengths = lengths.at[source_of].add(-moved).at[receiver].add(moved)
    items = jnp.searchsorted(jnp.cumsum(lengths), jnp.arange(rows * top), side="right").astype(jnp.int32)
    grid = items.reshape(top, rows).T
    grid = grid[jax.random.permutation(jax.random.fold_in(own, 1), rows)]
    turn = jax.random.randint(jax.random.fold_in(own, 2), (rows, 1), 0, top)
    return jnp.take_along_axis(grid, (jnp.arange(top)[None, :] + turn) % top, axis=1)


def shares(amount, total, most, lean, full):
    weights = [(1 << 20) // math.isqrt(grade ** lean) + 1 for grade in range(1, amount + 1)]
    largest = most if full else min(most, max(-(-total // amount), total * weights[0] // sum(weights)))
    least = 1 if total - largest >= amount - 1 else 0
    given, surplus = [largest] + [least] * (amount - 1), total - largest - least * (amount - 1)
    while surplus > 0:
        movable = [i for i in range(1, amount) if given[i] < largest] or [i for i in range(1, amount) if given[i] < most]
        pool, left = sum([weights[i] for i in movable]), surplus
        for i in movable:
            addition = min(most - given[i], max(1, left * weights[i] // pool), surplus)
            given[i] = given[i] + addition
            surplus = surplus - addition
    return np.array(given)


def normal_values(rng, shape, deviation, bound, cuts=(), kind=jnp.bfloat16):
    loudness = levels(rng, shape, cuts, -0.22, 0.18) if cuts else 1.0
    result = jax.random.normal(rng, shape, jnp.float32) * deviation * loudness
    return jnp.minimum(jnp.maximum(result, -bound), bound).astype(kind)


def setup_inputs(seed: int = 0) -> dict:
    splits = jax.random.split(jax.random.key(seed), 6)
    mixing = jnp.clip(jnp.exp(math.log(3.0) - 4.0943445 * jax.random.uniform(splits[0], (3, LEV, COLS), jnp.float32) ** levels(splits[0], (3, LEV, COLS), ((1, 4), (2, 8)), -0.2, 0.2)), 0.05, 3.0)
    density = jnp.clip(jnp.exp(math.log(1.2) - 1.0986123 * jax.random.uniform(splits[1], (LEV, COLS), jnp.float32) ** levels(splits[1], (LEV, COLS), ((0, 4), (1, 8)), -0.2, 0.2)), 0.4, 1.2)
    routes_keys = jax.random.split(jax.random.fold_in(splits[2], 1), COLS // COL_DEV)
    routes_turns = jax.random.permutation(jax.random.fold_in(splits[2], 3), COLS // COL_DEV)
    routes = jax.vmap(lambda own, number: deal_out(jax.random.fold_in(splits[2], 2), own, number, COL_DEV, N_TILE, 1, CAP, 2))(routes_keys, routes_turns).reshape((COLS, 1))
    beam_weight = jnp.clip(jnp.exp(math.log(0.06) - 4.0943445 * jax.random.uniform(splits[3], (SITES, GATE_COL, LEV), jnp.float32) ** levels(splits[3], (SITES, GATE_COL, LEV), ((0, 8),), -0.2, 0.2)), 0.001, 0.06)
    gate_adjoint = normal_values(splits[4], (GATE_COL, SLOTS), 1.0, 6.0, ((0, 4), (1, 8)), jnp.float32)
    return {"mixing": mixing, "density": density, "routes": routes, "beam_weight": beam_weight, "gate_adjoint": gate_adjoint}


coefficients = (3.63, 0.96, 1.98)
exponents = (1.75, 1.66, 1.75)


def reflect(mixing, density):
    summed = jnp.zeros(density.shape, jnp.float32)
    slopes = []
    for species in range(3):
        scaled = density * mixing[species]
        powered = coefficients[species] * jnp.exp(exponents[species] * jnp.log(scaled))
        summed = summed + powered
        slopes.append(exponents[species] * powered / mixing[species])
    return summed, jnp.stack(slopes)


def reference(mixing, density, routes, beam_weight, gate_adjoint):
    tile_count = N_TILE
    capacity = 2 * COL_DEV // tile_count
    slot_total = tile_count * capacity
    reflectivity, slopes = reflect(mixing, density)
    target = routes[:, 0].reshape(tile_count, COL_DEV).astype(jnp.int32)
    onehot = (target[:, :, None] == jnp.arange(tile_count, dtype=jnp.int32)[None, None, :]).astype(jnp.int32)
    ranking = jnp.sum((jnp.cumsum(onehot, axis=1) - onehot) * onehot, axis=2)
    source = jnp.arange(tile_count, dtype=jnp.int32)[:, None]
    position = (target * slot_total + source * capacity + ranking).reshape(-1).astype(jnp.int32)
    site_columns = jnp.zeros((LEV, tile_count * slot_total), jnp.float32).at[:, position].set(reflectivity)
    gate_values = jnp.einsum("dgl,ldk->gdk", beam_weight, site_columns.reshape(LEV, tile_count, slot_total),
                             precision=lax.Precision.HIGHEST).reshape(GATE_COL, tile_count * slot_total)
    site_adjoint = jnp.einsum("dgl,gdk->ldk", beam_weight, gate_adjoint.reshape(GATE_COL, tile_count, slot_total),
                              precision=lax.Precision.HIGHEST).reshape(LEV, tile_count * slot_total)
    increments = slopes * site_adjoint[:, position][None]
    return gate_values, increments
```

```python
import functools

import jax
import jax.numpy as jnp
from jax import lax
from jax.experimental import pallas as pl
from jax.experimental.pallas import tpu as pltpu
from jax.sharding import PartitionSpec as P

coefficients = (3.63, 0.96, 1.98)
exponents = (1.75, 1.66, 1.75)
LANES = 128
ROWS = 8
GROUP = 8
VMEM = pltpu.VMEM
SMEM = pltpu.SMEM


def iota(shape, dim):
    return lax.broadcasted_iota(jnp.int32, shape, dim)


def halves(x):
    high = x.astype(jnp.bfloat16)
    low = (x - high.astype(jnp.float32)).astype(jnp.bfloat16)
    return high, low


def split_dot(weights, x):
    w_high, w_low = halves(weights)
    x_high, x_low = halves(x)
    rows = weights.shape[0]
    both = jnp.dot(jnp.concatenate([w_high, w_low], 0), x_high, preferred_element_type=jnp.float32)
    rest = jnp.dot(w_high, x_low, preferred_element_type=jnp.float32)
    return both[:rows] + (both[rows:] + rest)


def rank_kernel(targets, t_ref, rank_ref, sorted_ref, offset_ref, start_ref):
    blocks = t_ref.shape[0]
    t = t_ref[...]
    before = (iota((LANES, LANES), 0) <= iota((LANES, LANES), 1)).astype(jnp.float32)
    sums = jnp.concatenate([before, jnp.ones((LANES, LANES), jnp.float32)], 1).astype(jnp.bfloat16)
    earlier = (iota((offset_ref.shape[0], blocks), 1) < iota((offset_ref.shape[0], blocks), 0))
    earlier = earlier.astype(jnp.float32).astype(jnp.bfloat16)
    lane = iota((1, LANES), 1)
    start = jnp.zeros((blocks, LANES), jnp.float32)
    rank = jnp.zeros((blocks, LANES), jnp.float32)
    place = jnp.zeros((blocks, LANES), jnp.float32)
    starts = jnp.zeros((blocks, LANES), jnp.float32)
    offsets = jnp.zeros(offset_ref.shape, jnp.float32)
    for first in range(0, targets, GROUP):
        group = range(first, min(first + GROUP, targets))
        masks = [t == d for d in group]
        ones = jnp.concatenate([m.astype(jnp.float32) for m in masks], 0).astype(jnp.bfloat16)
        counted = jnp.dot(ones, sums, preferred_element_type=jnp.float32)
        totals = [counted[i * blocks:(i + 1) * blocks, LANES:] for i in range(len(masks))]
        based = jnp.dot(earlier, jnp.concatenate(totals, 1).astype(jnp.bfloat16), preferred_element_type=jnp.float32)
        for i, d in enumerate(group):
            inclusive = counted[i * blocks:(i + 1) * blocks, :LANES]
            base = based[:, i * LANES:(i + 1) * LANES]
            rank = jnp.where(masks[i], base[:blocks] + inclusive - 1.0, rank)
            place = jnp.where(masks[i], start + inclusive - 1.0, place)
            starts = jnp.where(lane == d, start, starts)
            offsets = jnp.where(lane == d, base, offsets)
            start = start + totals[i]
    rank_ref[...] = rank.astype(jnp.int32)
    sorted_ref[...] = place.astype(jnp.int32)
    start_ref[...] = starts.astype(jnp.int32)
    offset_ref[...] = offsets.astype(jnp.int32)


def reflect_kernel(offset_ref, start_ref, mixing_ref, density_ref, place_ref, out_ref, slope_ref, sorted_ref):
    targets, levels, capacity = out_ref.shape
    blocks = place_ref.shape[0]
    tiles = capacity // LANES
    lanes_row = iota((ROWS, LANES), 1).astype(jnp.float32).astype(jnp.bfloat16)
    sublane = iota((LANES, LANES), 0)
    lane = iota((levels, LANES), 1)

    def reflect(j, carry):
        at = pl.ds(pl.multiple_of(j * LANES, LANES), LANES)
        rho = density_ref[:, at]
        total = jnp.zeros((levels, LANES), jnp.float32)
        for k in range(3):
            q = mixing_ref[k, :, at]
            powered = coefficients[k] * jnp.exp(exponents[k] * jnp.log(rho * q))
            total = total + powered
            slope_ref[k, :, at] = exponents[k] * powered / q
        place = place_ref[pl.ds(j, 1), :]
        chosen = (sublane == place).astype(jnp.float32).astype(jnp.bfloat16)
        source = lax.dot_general(lanes_row, chosen, (((1,), (1,)), ((), ())), preferred_element_type=jnp.float32)
        source = source.astype(jnp.int32)
        for r in range(0, levels, ROWS):
            sorted_ref[r:r + ROWS, at] = jnp.take_along_axis(total[r:r + ROWS], source, axis=1)
        return carry

    lax.fori_loop(0, blocks, reflect, 0, unroll=4)
    out_ref[...] = jnp.zeros(out_ref.shape, jnp.float32)

    def place_group(first, count):
        def step(j, held):
            at = pl.ds(pl.multiple_of(j * LANES, LANES), LANES)
            values = sorted_ref[:, at]
            new = []
            for i in range(count):
                d = first + i
                offset = offset_ref[j, d]
                number = offset_ref[j + 1, d] - offset
                low = offset & (LANES - 1)
                end = low + number
                tile = jnp.minimum(offset // LANES, tiles - 1)
                turned = pltpu.roll(values, (low - start_ref[j, d]) & (LANES - 1), 1)
                merged = jnp.where((lane >= low) & (lane < end), turned, held[i])
                out_ref[d, :, pl.ds(pl.multiple_of(tile * LANES, LANES), LANES)] = merged
                full = (end >= LANES) & (tile + 1 < tiles)
                spill = jnp.where(full, end - LANES, 0)
                new.append(jnp.where(lane < spill, turned, jnp.where(full, 0.0, merged)))
            return tuple(new)

        zero = jnp.zeros((levels, LANES), jnp.float32)
        held = lax.fori_loop(0, blocks, step, (zero,) * count)
        for i in range(count):
            d = first + i
            tile = jnp.minimum(offset_ref[blocks, d] // LANES, tiles - 1)
            out_ref[d, :, pl.ds(pl.multiple_of(tile * LANES, LANES), LANES)] = held[i]

    count = min(GROUP, targets)
    if targets <= count:
        place_group(0, count)
    else:
        @pl.loop(0, targets // count)
        def _(g):
            place_group(g * count, count)


def adjoint_kernel(w_ref, own_ref, near_ref, *out_refs):
    total = split_dot(w_ref[0], own_ref[...]) + split_dot(w_ref[1], near_ref[...])
    levels = out_refs[0].shape[1]
    for i, out_ref in enumerate(out_refs):
        out_ref[0] = total[i * levels:(i + 1) * levels]


def gate_kernel(w_ref, *refs):
    out_ref = refs[-1]
    parts = [ref[0] if len(ref.shape) == 3 else ref[0, 0] for ref in refs[:-1]]
    out_ref[...] = split_dot(w_ref[...], jnp.concatenate(parts, 0))


def increment_kernel(offset_ref, back_ref, rank_ref, t_ref, slope_ref, out_ref):
    targets, levels, capacity = back_ref.shape
    blocks = rank_ref.shape[0]
    tiles = capacity // LANES
    lane = iota((levels, LANES), 1)
    count = min(GROUP, targets)

    def block(j, carry):
        at = pl.ds(pl.multiple_of(j * LANES, LANES), LANES)
        index = jnp.broadcast_to(rank_ref[pl.ds(j, 1), :] & (LANES - 1), (ROWS, LANES))
        target = jnp.broadcast_to(t_ref[pl.ds(j, 1), :], (levels, LANES))

        def pick(first, found):
            for i in range(count):
                d = first + i
                offset = offset_ref[j, d]
                tile = jnp.minimum(offset // LANES, tiles - 1)
                later = jnp.minimum(tile + 1, tiles - 1)
                one = back_ref[d, :, pl.ds(pl.multiple_of(tile * LANES, LANES), LANES)]
                two = back_ref[d, :, pl.ds(pl.multiple_of(later * LANES, LANES), LANES)]
                window = jnp.where(lane >= (offset & (LANES - 1)), one, two)
                moved = [jnp.take_along_axis(window[r:r + ROWS], index, axis=1) for r in range(0, levels, ROWS)]
                found = jnp.where(target == d, jnp.concatenate(moved, 0), found)
            return found

        found = jnp.zeros((levels, LANES), jnp.float32)
        if targets <= count:
            found = pick(0, found)
        else:
            found = lax.fori_loop(0, targets // count, lambda g, f: pick(g * count, f), found)
        for k in range(3):
            out_ref[k, :, at] = slope_ref[k, :, at] * found
        return carry

    lax.fori_loop(0, blocks, block, 0, unroll=2)


def full(space=VMEM):
    return pl.BlockSpec(memory_space=space)


def per_device(mixing, density, routes, beam_weight, gate_adjoint):
    tile_count = lax.axis_size("tile")
    level_count = lax.axis_size("lev")
    me = lax.axis_index("lev")
    level_dev, column_dev = density.shape
    capacity = 2 * column_dev // tile_count
    blocks = column_dev // LANES
    far = level_count // 2
    gate_dev = gate_adjoint.shape[0]
    f32 = jnp.float32

    def swap(x, bits):
        return lax.ppermute(x, "lev", [(i, i ^ bits) for i in range(level_count)])

    near_adjoint = swap(gate_adjoint, 1)

    t = routes.reshape(blocks, LANES)
    i32 = functools.partial(jax.ShapeDtypeStruct, dtype=jnp.int32)
    rank, place, offsets, starts = pl.pallas_call(
        functools.partial(rank_kernel, tile_count),
        out_shape=(i32((blocks, LANES)), i32((blocks, LANES)), i32((blocks + ROWS, LANES)), i32((blocks, LANES))),
        in_specs=[full()],
        out_specs=[full()] * 4,
        name="rank",
    )(t)
    outgoing, slopes = pl.pallas_call(
        reflect_kernel,
        out_shape=(
            jax.ShapeDtypeStruct((tile_count, level_dev, capacity), f32),
            jax.ShapeDtypeStruct(mixing.shape, f32),
        ),
        in_specs=[full(SMEM), full(SMEM), full(), full(), full()],
        out_specs=[full(), full()],
        scratch_shapes=[pltpu.VMEM((level_dev, column_dev), f32)],
        name="reflect",
    )(offsets, starts, mixing, density, place)

    by_level = beam_weight[0].T.reshape(level_count, level_dev, level_count, gate_dev)
    level_order = [me ^ (2 * m) for m in range(far)]
    adjoint_weights = jnp.stack([
        jnp.concatenate([by_level[l, :, g, :] for l in level_order], 0) for g in (me, me ^ 1)
    ])
    block_spec = pl.BlockSpec((1, level_dev, capacity), lambda s: (s, 0, 0))
    slot_spec = pl.BlockSpec((gate_dev, capacity), lambda s: (0, s))
    partial = pl.pallas_call(
        adjoint_kernel,
        grid=(tile_count,),
        out_shape=[jax.ShapeDtypeStruct((tile_count, level_dev, capacity), f32)] * far,
        in_specs=[pl.BlockSpec(adjoint_weights.shape, lambda s: (0, 0, 0)), slot_spec, slot_spec],
        out_specs=[block_spec] * far,
        name="adjoint",
    )(adjoint_weights, gate_adjoint, near_adjoint)
    returned = partial[0]
    for m in range(1, far):
        returned = returned + swap(partial[m], 2 * m)

    incoming = lax.all_to_all(outgoing, "tile", split_axis=0, concat_axis=0, tiled=True)
    held = [incoming] + [swap(incoming, 2 * m) for m in range(1, far)]
    near = swap(jnp.stack(held), 1)
    restored = lax.all_to_all(returned, "tile", split_axis=0, concat_axis=0, tiled=True)

    order = level_order + [l ^ 1 for l in level_order]
    gate_weights = jnp.concatenate([by_level[l, :, me, :].T for l in order], 1)
    near_specs = [pl.BlockSpec((1, 1, level_dev, capacity), lambda s, m=m: (m, s, 0, 0)) for m in range(far)]
    gate_values = pl.pallas_call(
        gate_kernel,
        grid=(tile_count,),
        out_shape=jax.ShapeDtypeStruct(gate_adjoint.shape, f32),
        in_specs=[pl.BlockSpec(gate_weights.shape, lambda s: (0, 0))] + [block_spec] * far + near_specs,
        out_specs=slot_spec,
        name="gates",
    )(gate_weights, *held, *([near] * far))
    increments = pl.pallas_call(
        increment_kernel,
        out_shape=jax.ShapeDtypeStruct(mixing.shape, f32),
        in_specs=[full(SMEM), full(), full(), full(), full()],
        out_specs=full(),
        name="increments",
    )(offsets, restored, rank, t, slopes)
    return gate_values, increments


def solution(mesh):
    return jax.shard_map(
        per_device,
        mesh=mesh,
        in_specs=(
            P(None, "lev", "tile"),
            P("lev", "tile"),
            P("tile", None),
            P("tile", None, None),
            P("lev", "tile"),
        ),
        out_specs=(P("lev", "tile"), P(None, "lev", "tile")),
        check_vma=False,
    )
```

```python
import functools

import jax
import jax.numpy as jnp
from jax import lax
from jax.experimental import pallas as pl
from jax.experimental.pallas import tpu as pltpu
from jax.sharding import PartitionSpec as P

coefficients = (3.63, 0.96, 1.98)
exponents = (1.75, 1.66, 1.75)
LANES = 128
ROWS = 8
GROUP = 8
DIRECT = 8
SMEM = pltpu.SMEM


def iota(shape, dim):
    return lax.broadcasted_iota(jnp.int32, shape, dim)


def tile_at(index):
    return pl.ds(pl.multiple_of(index * LANES, LANES), LANES)


def halves(x):
    high = x.astype(jnp.bfloat16)
    low = (x - high.astype(jnp.float32)).astype(jnp.bfloat16)
    return high, low


def split_dot(weights, x):
    w_high, w_low = halves(weights)
    x_high, x_low = halves(x)
    rows = weights.shape[0]
    both = jnp.dot(jnp.concatenate([w_high, w_low], 0), x_high, preferred_element_type=jnp.float32)
    rest = jnp.dot(w_high, x_low, preferred_element_type=jnp.float32)
    return both[:rows] + (both[rows:] + rest)


def first_target(targets):
    return lax.axis_index("tile") if targets <= DIRECT else 0


def blocks_of(refs):
    return [ref.at[i] for ref in refs if len(ref.shape) == 3 for i in range(ref.shape[0])] or list(refs)


def low_of(word):
    return (jnp.full((ROWS, LANES), word, jnp.int32) >> 7) & 255


def keep_of(word):
    return (jnp.full((ROWS, LANES), word, jnp.int32) >> 15) & 255


def rank_kernel(targets, tiles, t_ref, table_ref, rank_ref, place_ref):
    t = t_ref[...]
    me = first_target(targets)
    blocks = t.shape[0]
    rows = blocks + ROWS
    before = (iota((LANES, LANES), 0) <= iota((LANES, LANES), 1)).astype(jnp.float32)
    sums = jnp.concatenate([before, jnp.ones((LANES, LANES), jnp.float32)], 1).astype(jnp.bfloat16)
    earlier = (iota((rows, blocks), 1) < iota((rows, blocks), 0)).astype(jnp.float32).astype(jnp.bfloat16)
    lane = iota((1, LANES), 1)
    start = jnp.zeros((blocks, LANES), jnp.float32)
    rank = jnp.zeros((blocks, LANES), jnp.float32)
    place = jnp.zeros((blocks, LANES), jnp.float32)
    starts = jnp.zeros((blocks, LANES), jnp.float32)
    numbers = jnp.zeros((blocks, LANES), jnp.float32)
    offsets = jnp.zeros((rows, LANES), jnp.float32)
    for first in range(0, targets, GROUP):
        group = range(first, min(first + GROUP, targets))
        masks = [t == d for d in group]
        ones = jnp.concatenate([m.astype(jnp.float32) for m in masks], 0).astype(jnp.bfloat16)
        counted = jnp.dot(ones, sums, preferred_element_type=jnp.float32)
        totals = [counted[i * blocks:(i + 1) * blocks, LANES:] for i in range(len(masks))]
        based = jnp.dot(earlier, jnp.concatenate(totals, 1).astype(jnp.bfloat16), preferred_element_type=jnp.float32)
        for i, d in enumerate(group):
            inclusive = counted[i * blocks:(i + 1) * blocks, :LANES]
            base = based[:, i * LANES:(i + 1) * LANES]
            mine = lane % targets == d ^ me
            rank = jnp.where(masks[i], base[:blocks] + inclusive - 1.0, rank)
            place = jnp.where(masks[i], start + inclusive - 1.0, place)
            starts = jnp.where(mine, start, starts)
            numbers = jnp.where(mine, totals[i], numbers)
            offsets = jnp.where(mine, base, offsets)
            start = start + totals[i]
    pad = jnp.zeros((rows - blocks, LANES), jnp.int32)
    starts = jnp.concatenate([starts.astype(jnp.int32), pad], 0)
    numbers = jnp.concatenate([numbers.astype(jnp.int32), pad], 0)
    offsets = offsets.astype(jnp.int32)
    tile = jnp.minimum(offsets >> 7, tiles - 1)
    low = jnp.where(offsets == tiles * LANES, LANES, offsets & (LANES - 1))
    keep = jnp.where((low + numbers >= LANES) & (tile + 1 < tiles), 0, low)
    turn = (low - starts) & (LANES - 1)
    word = turn + (low << 7) + (keep << 15) + (tile << 23)
    word = jnp.concatenate([word, jnp.zeros((LANES - rows, LANES), jnp.int32)], 0)
    table_ref[...] = word.T[:table_ref.shape[0]]
    rank_ref[...] = rank.astype(jnp.int32)
    place_ref[...] = place.astype(jnp.int32)


def source_kernel(targets, table_ref, place_ref, mixing_ref, density_ref, *refs):
    slope_ref, outs = refs[0], blocks_of(refs[1:-3])
    sorted_ref, table_smem, table_sem = refs[-3:]
    levels, capacity = outs[0].shape
    blocks = place_ref.shape[0]
    load_table = pltpu.make_async_copy(table_ref, table_smem, table_sem)
    load_table.start()
    lanes_row = iota((ROWS, LANES), 1).astype(jnp.float32).astype(jnp.bfloat16)
    sublane = iota((LANES, LANES), 0)
    lane = iota((ROWS, LANES), 1)
    parts = range(0, levels, ROWS)
    for out in outs:
        out[...] = jnp.zeros((levels, capacity), jnp.float32)

    def reflect(j, carry):
        at = tile_at(j)
        rho = density_ref[:, at]
        total = jnp.zeros((levels, LANES), jnp.float32)
        for k in range(3):
            q = mixing_ref[k, :, at]
            powered = coefficients[k] * jnp.exp(exponents[k] * jnp.log(rho * q))
            total = total + powered
            slope_ref[k, :, at] = exponents[k] * powered / q
        chosen = (sublane == place_ref[pl.ds(j, 1), :]).astype(jnp.float32).astype(jnp.bfloat16)
        source = lax.dot_general(lanes_row, chosen, (((1,), (1,)), ((), ())), preferred_element_type=jnp.float32)
        source = source.astype(jnp.int32)
        for r in parts:
            sorted_ref[r:r + ROWS, at] = jnp.take_along_axis(total[r:r + ROWS], source, axis=1)
        return carry

    lax.fori_loop(0, blocks, reflect, 0, unroll=4)
    load_table.wait()

    def place_group(first, count):
        def step(j, held):
            values = [sorted_ref[r:r + ROWS, tile_at(j)] for r in parts]
            new = []
            for i in range(count):
                word = table_smem[first + i, j]
                low, keep, turn, at = low_of(word), keep_of(word), word & (LANES - 1), tile_at(word >> 23)
                for n, r in enumerate(parts):
                    turned = pltpu.roll(values[n], turn, 1)
                    out = refs[1].at[first + i] if targets > DIRECT else outs[i]
                    out[r:r + ROWS, at] = jnp.where(lane >= low, turned, held[i * len(parts) + n])
                    new.append(jnp.where(lane >= keep, turned, held[i * len(parts) + n]))
            return tuple(new)

        zero = jnp.zeros((ROWS, LANES), jnp.float32)
        held = lax.fori_loop(0, blocks, step, (zero,) * (count * len(parts)), unroll=2)
        for i in range(count):
            out = refs[1].at[first + i] if targets > DIRECT else outs[i]
            word = table_smem[first + i, blocks]
            for n, r in enumerate(parts):
                out[r:r + ROWS, tile_at(word >> 23)] = jnp.where(lane < low_of(word), held[i * len(parts) + n], 0.0)

    if targets <= GROUP:
        place_group(0, targets)
    else:
        @pl.loop(0, targets // GROUP)
        def _(g):
            place_group(g * GROUP, GROUP)


def pick_weights(w_ref, picked_ref, order, rows):
    gates = picked_ref.shape[-1]
    levels = picked_ref.shape[0] // len(order)
    for part in range(w_ref.shape[1] // gates):
        @pl.when(rows == part)
        def _():
            for i, l in enumerate(order):
                block = w_ref[pl.ds(pl.multiple_of(l * levels, levels), levels), :]
                picked_ref[i * levels:(i + 1) * levels, :] = block[:, part * gates:(part + 1) * gates]


def adjoint_kernel(targets, group, w_ref, own_ref, near_ref, *refs):
    out_refs, picked_ref = refs[:-1], refs[-1]
    levels, capacity = out_refs[0].shape[1:]
    me = first_target(targets)
    mine = lax.axis_index("lev")
    order = [mine ^ (2 * m) for m in range(len(out_refs))]
    for i in range(2):
        pick_weights(w_ref, picked_ref.at[i], order, mine ^ i)

    def step(s, carry):
        at = (group.start + group.step * s) ^ me
        at = pl.ds(pl.multiple_of(at * capacity, capacity), capacity)
        total = split_dot(picked_ref[0], own_ref[:, at]) + split_dot(picked_ref[1], near_ref[:, at])
        for i, out_ref in enumerate(out_refs):
            out_ref[s] = total[i * levels:(i + 1) * levels]
        return carry

    lax.fori_loop(0, len(group), step, 0)


def gate_part(targets, group, w_ref, sources, out_any, buffer, picked_ref, sem):
    mine = lax.axis_index("lev")
    half = len(sources) // 2
    order = [mine ^ (2 * (i % half)) ^ (i // half) for i in range(len(sources))]
    pick_weights(w_ref, picked_ref, order, mine)
    capacity = sources[0].shape[-1]
    me = first_target(targets)
    weights = picked_ref[...].T

    def column(s):
        return pl.ds(pl.multiple_of(((group.start + group.step * s) ^ me) * capacity, capacity), capacity)

    def store(s):
        part = pl.ds(pl.multiple_of(s * capacity, capacity), capacity)
        return pltpu.make_async_copy(buffer.at[:, part], out_any.at[:, column(s)], sem.at[s])

    def step(s, carry):
        part = pl.ds(pl.multiple_of(s * capacity, capacity), capacity)
        buffer[:, part] = split_dot(weights, jnp.concatenate([ref[s] for ref in sources], 0))
        store(s).start()
        return carry

    def finish(s, carry):
        store(s).wait()
        return carry

    lax.fori_loop(0, len(group), step, 0)
    return lambda: lax.fori_loop(0, len(group), finish, 0)


def increment_part(targets, table_ref, rank_ref, t_ref, slope_ref, refs, out_any, out_ref, sem):
    backs = blocks_of(refs)
    levels, capacity = backs[0].shape
    blocks = rank_ref.shape[0]
    tiles = capacity // LANES
    lane = iota((ROWS, LANES), 1)
    parts = range(0, levels, ROWS)
    me = first_target(targets)
    count = min(GROUP, targets)

    def block(j, carry):
        index = jnp.broadcast_to(rank_ref[pl.ds(j, 1), :] & (LANES - 1), (ROWS, LANES))
        target = jnp.broadcast_to(t_ref[pl.ds(j, 1), :], (ROWS, LANES)) ^ me

        def pick(first, found):
            found = list(found)
            for i in range(count):
                word = table_ref[first + i, j]
                low, tile = low_of(word), word >> 23
                later = jnp.minimum(tile + 1, tiles - 1)
                back = refs[0].at[first + i] if targets > DIRECT else backs[i]
                for n, r in enumerate(parts):
                    window = jnp.where(lane >= low, back[r:r + ROWS, tile_at(tile)], back[r:r + ROWS, tile_at(later)])
                    moved = jnp.take_along_axis(window, index, axis=1)
                    found[n] = jnp.where(target == first + i, moved, found[n])
            return tuple(found)

        found = (jnp.zeros((ROWS, LANES), jnp.float32),) * len(parts)
        if targets <= count:
            found = pick(0, found)
        else:
            found = lax.fori_loop(0, targets // count, lambda g, f: pick(g * count, f), found)
        for k in range(3):
            for n, r in enumerate(parts):
                out_ref[k, r:r + ROWS, tile_at(j)] = slope_ref[k, r:r + ROWS, tile_at(j)] * found[n]
        return carry

    pieces = sem.shape[0]
    stores = []
    for p in range(pieces):
        first, last = blocks * p // pieces, blocks * (p + 1) // pieces
        lax.fori_loop(first, last, block, 0, unroll=4)
        here = slice(first * LANES, last * LANES)
        stores.append(pltpu.make_async_copy(out_ref.at[:, :, here], out_any.at[:, :, here], sem.at[p]))
        stores[-1].start()
    return lambda: [store.wait() for store in stores]


def gate_kernel(targets, group, w_ref, *refs):
    out_any, buffer, picked_ref, sem = refs[-4:]
    sources = [ref for ref in refs[:-4] if len(ref.shape) == 3]
    gate_part(targets, group, w_ref, sources, out_any, buffer, picked_ref, sem)()


def final_kernel(targets, group, columns, backs, table_ref, rank_ref, t_ref, slope_ref, w_ref, *refs):
    sources, refs = refs[:columns], refs[columns:]
    returned, refs = refs[:backs], refs[backs:]
    gate_any, out_any, buffer, picked_ref, gate_sem, out_ref, out_sem = refs[-7:]
    gates_done = gate_part(targets, group, w_ref, sources, gate_any, buffer, picked_ref, gate_sem)
    increments_done = increment_part(
        targets, table_ref, rank_ref, t_ref, slope_ref, returned, out_any, out_ref, out_sem)
    gates_done()
    increments_done()


def settings(mib, micros):
    cost = pl.CostEstimate(flops=int(micros * 1e9), bytes_accessed=0, transcendentals=0)
    return dict(compiler_params=pltpu.CompilerParams(vmem_limit_bytes=mib << 20), cost_estimate=cost)


def full(space=pltpu.VMEM):
    return pl.BlockSpec(memory_space=space)


def per_device(mixing, density, routes, beam_weight, gate_adjoint):
    tile_count = lax.axis_size("tile")
    level_count = lax.axis_size("lev")
    level_dev, column_dev = density.shape
    capacity = 2 * column_dev // tile_count
    blocks = column_dev // LANES
    far = level_count // 2
    gate_dev = gate_adjoint.shape[0]
    direct = tile_count <= DIRECT
    f32, i32 = jnp.float32, jnp.int32
    shape = jax.ShapeDtypeStruct

    def swap(x, bits):
        return lax.ppermute(x, "lev", [(i, i ^ bits) for i in range(level_count)])

    def exchange(x, bits):
        return lax.ppermute(x, "tile", [(i, i ^ bits) for i in range(tile_count)])

    weights = beam_weight[0].T
    t = routes.reshape(blocks, LANES)
    table_shape = (max(tile_count, ROWS), LANES)
    half = tile_count // 2
    if direct:
        block_shapes = [shape((level_dev, capacity), f32)] * tile_count
        groups = [range(1, tile_count, 2), range(0, tile_count, 2)]
        sites = [range(0, half), range(half, tile_count)]
    else:
        block_shapes = [shape((tile_count, level_dev, capacity), f32)]
        groups = sites = [range(0, tile_count)]

    near_adjoint = swap(gate_adjoint, 1)
    table, rank, place = pl.pallas_call(
        functools.partial(rank_kernel, tile_count, capacity // LANES),
        out_shape=[shape(table_shape, i32)] + [shape((blocks, LANES), i32)] * 2,
        in_specs=[full()],
        out_specs=[full()] * 3,
        **settings(12, 1),
    )(t)
    slopes, *outgoing = pl.pallas_call(
        functools.partial(source_kernel, tile_count),
        out_shape=[shape(mixing.shape, f32)] + block_shapes,
        in_specs=[full()] * 4,
        out_specs=[full()] * (1 + len(block_shapes)),
        scratch_shapes=[
            pltpu.VMEM(density.shape, f32),
            pltpu.SMEM(table_shape, i32),
            pltpu.SemaphoreType.DMA,
        ],
        **settings(12, 4),
    )(table, place, mixing, density)

    partial = []
    for group in groups:
        partial.append(pl.pallas_call(
            functools.partial(adjoint_kernel, tile_count, group),
            out_shape=[shape((len(group), level_dev, capacity), f32)] * far,
            in_specs=[full()] * 3,
            out_specs=[full()] * far,
            scratch_shapes=[pltpu.VMEM((2, far * level_dev, gate_dev), f32)],
            **settings(12, 2),
        )(weights, gate_adjoint, near_adjoint))

    totals = []
    for parts in partial:
        total = parts[0]
        for m in range(1, far):
            part = swap(parts[m], 2 * m)
            total = total + part
        totals.append(total)
    if direct:
        incoming = [outgoing[0]]
        for k in range(1, tile_count):
            incoming.append(exchange(outgoing[k], k))
        arrived = []
        for site in sites:
            arrived.append(jnp.stack([incoming[k] for k in site]))
        crossed = exchange(totals[0], 1)
        restored = []
        for p in range(half):
            pair = jnp.stack([totals[1][p], crossed[p]])
            restored.append(pair if p == 0 else exchange(pair, 2 * p))
    else:
        arrived = [lax.all_to_all(outgoing[0], "tile", split_axis=0, concat_axis=0, tiled=True)]
        restored = [lax.all_to_all(totals[0], "tile", split_axis=0, concat_axis=0, tiled=True)]

    gate_values = None
    for n, (group, here) in enumerate(zip(sites, arrived)):
        columns = [here]
        for m in range(1, far):
            columns.append(swap(here, 2 * m))
        for m in range(far):
            columns.append(swap(columns[m], 1))
        before = [] if gate_values is None else [gate_values]
        gate_scratch = [
            pltpu.VMEM((gate_dev, len(group) * capacity), f32),
            pltpu.VMEM(weights.shape[:1] + (gate_dev,), f32),
            pltpu.SemaphoreType.DMA((len(group),)),
        ]
        if n + 1 < len(sites):
            gate_values = pl.pallas_call(
                functools.partial(gate_kernel, tile_count, group),
                out_shape=shape(gate_adjoint.shape, f32),
                in_specs=[full()] * (1 + len(columns)) + [full(pltpu.HBM)] * len(before),
                out_specs=full(pltpu.HBM),
                input_output_aliases={1 + len(columns): 0} if before else {},
                scratch_shapes=gate_scratch,
                **settings(12, 2),
            )(weights, *columns, *before)
            continue
        operands = [table, rank, t, slopes, weights, *columns, *restored]
        gate_values, increments = pl.pallas_call(
            functools.partial(final_kernel, tile_count, group, len(columns), len(restored)),
            out_shape=[shape(gate_adjoint.shape, f32), shape(mixing.shape, f32)],
            in_specs=[full(SMEM)] + [full()] * (len(operands) - 1) + [full(pltpu.HBM)] * len(before),
            out_specs=[full(pltpu.HBM)] * 2,
            input_output_aliases={len(operands): 0} if before else {},
            scratch_shapes=gate_scratch + [pltpu.VMEM(mixing.shape, f32), pltpu.SemaphoreType.DMA((4,))],
            **settings(16, 4),
        )(*operands, *before)
    return gate_values, increments


def solution(mesh):
    return jax.shard_map(
        per_device,
        mesh=mesh,
        in_specs=(
            P(None, "lev", "tile"),
            P("lev", "tile"),
            P("tile", None),
            P("tile", None, None),
            P("lev", "tile"),
        ),
        out_specs=(P("lev", "tile"), P(None, "lev", "tile")),
        check_vma=False,
    )
```

```python
import functools

import jax
import jax.numpy as jnp
from jax import lax
from jax.experimental import pallas as pl
from jax.experimental.pallas import tpu as pltpu
from jax.sharding import PartitionSpec as P

coefficients = (3.63, 0.96, 1.98)
exponents = (1.75, 1.66, 1.75)
LANES = 128
ROWS = 8
GROUP = 8
DIRECT = 8
SMEM = pltpu.SMEM


def iota(shape, dim):
    return lax.broadcasted_iota(jnp.int32, shape, dim)


def tile_at(index):
    if isinstance(index, int):
        return slice(index * LANES, (index + 1) * LANES)
    return pl.ds(pl.multiple_of(index * LANES, LANES), LANES)


def halves(x):
    high = x.astype(jnp.bfloat16)
    low = (x - high.astype(jnp.float32)).astype(jnp.bfloat16)
    return high, low


def split_dot(weights, x):
    w_high, w_low = halves(weights)
    x_high, x_low = halves(x)
    rows = weights.shape[0]
    both = jnp.dot(jnp.concatenate([w_high, w_low], 0), x_high, preferred_element_type=jnp.float32)
    rest = jnp.dot(w_high, x_low, preferred_element_type=jnp.float32)
    return both[:rows] + (both[rows:] + rest)


def first_target(targets):
    return lax.axis_index("tile") if targets <= DIRECT else 0


def blocks_of(refs):
    return [ref.at[i] for ref in refs if len(ref.shape) == 3 for i in range(ref.shape[0])] or list(refs)


def tile_of(word):
    return (word >> 23) & 31


def low_of(word):
    return (jnp.full((ROWS, LANES), word, jnp.int32) >> 7) & 255


def keep_of(word):
    return (jnp.full((ROWS, LANES), word, jnp.int32) >> 15) & 255


def rank_kernel(targets, tiles, t_ref, table_ref, rank_ref, place_ref):
    t = t_ref[...]
    me = first_target(targets)
    blocks = t.shape[0]
    rows = blocks + ROWS
    before = (iota((LANES, LANES), 0) <= iota((LANES, LANES), 1)).astype(jnp.float32)
    sums = jnp.concatenate([before, jnp.ones((LANES, LANES), jnp.float32)], 1).astype(jnp.bfloat16)
    earlier = (iota((rows, blocks), 1) < iota((rows, blocks), 0)).astype(jnp.float32).astype(jnp.bfloat16)
    lane = iota((1, LANES), 1)
    start = jnp.zeros((blocks, LANES), jnp.float32)
    rank = jnp.zeros((blocks, LANES), jnp.float32)
    place = jnp.zeros((blocks, LANES), jnp.float32)
    starts = jnp.zeros((blocks, LANES), jnp.float32)
    numbers = jnp.zeros((blocks, LANES), jnp.float32)
    offsets = jnp.zeros((rows, LANES), jnp.float32)
    for first in range(0, targets, GROUP):
        group = range(first, min(first + GROUP, targets))
        masks = [t == d for d in group]
        ones = jnp.concatenate([m.astype(jnp.float32) for m in masks], 0).astype(jnp.bfloat16)
        counted = jnp.dot(ones, sums, preferred_element_type=jnp.float32)
        totals = [counted[i * blocks:(i + 1) * blocks, LANES:] for i in range(len(masks))]
        based = jnp.dot(earlier, jnp.concatenate(totals, 1).astype(jnp.bfloat16), preferred_element_type=jnp.float32)
        for i, d in enumerate(group):
            inclusive = counted[i * blocks:(i + 1) * blocks, :LANES]
            base = based[:, i * LANES:(i + 1) * LANES]
            mine = lane % targets == d ^ me
            rank = jnp.where(masks[i], base[:blocks] + inclusive - 1.0, rank)
            place = jnp.where(masks[i], start + inclusive - 1.0, place)
            starts = jnp.where(mine, start, starts)
            numbers = jnp.where(mine, totals[i], numbers)
            offsets = jnp.where(mine, base, offsets)
            start = start + totals[i]
    pad = jnp.zeros((rows - blocks, LANES), jnp.int32)
    starts = jnp.concatenate([starts.astype(jnp.int32), pad], 0)
    numbers = jnp.concatenate([numbers.astype(jnp.int32), pad], 0)
    offsets = offsets.astype(jnp.int32)
    tile = jnp.minimum(offsets >> 7, tiles - 1)
    low = jnp.where(offsets == tiles * LANES, LANES, offsets & (LANES - 1))
    keep = jnp.where((low + numbers >= LANES) & (tile + 1 < tiles), 0, low)
    turn = (low - starts) & (LANES - 1)
    later = jnp.minimum(tile + 1, tiles - 1)
    word = turn | (low << 7) | (keep << 15) | (tile << 23) | (later << 28)
    word = jnp.concatenate([word, jnp.zeros((LANES - rows, LANES), jnp.int32)], 0)
    table_ref[...] = word.T[:table_ref.shape[0]]
    rank_ref[...] = rank.astype(jnp.int32)
    place_ref[...] = place.astype(jnp.int32)


def source_kernel(targets, table_ref, place_ref, mixing_ref, density_ref, *refs):
    slope_ref, outs = refs[0], blocks_of(refs[1:-3])
    sorted_ref, table_smem, table_sem = refs[-3:]
    levels, capacity = outs[0].shape
    blocks = place_ref.shape[0]
    load_table = pltpu.make_async_copy(table_ref, table_smem, table_sem)
    load_table.start()
    lanes_row = iota((ROWS, LANES), 1).astype(jnp.float32).astype(jnp.bfloat16)
    sublane = iota((LANES, LANES), 0)
    lane = iota((ROWS, LANES), 1)
    parts = range(0, levels, ROWS)
    for out in outs:
        out[...] = jnp.zeros((levels, capacity), jnp.float32)

    def reflect(j, carry):
        at = tile_at(j)
        rho = density_ref[:, at]
        total = jnp.zeros((levels, LANES), jnp.float32)
        for k in range(3):
            q = mixing_ref[k, :, at]
            powered = coefficients[k] * jnp.exp(exponents[k] * jnp.log(rho * q))
            total = total + powered
            slope_ref[k, :, at] = exponents[k] * powered / q
        chosen = (sublane == place_ref[pl.ds(j, 1), :]).astype(jnp.float32).astype(jnp.bfloat16)
        source = lax.dot_general(lanes_row, chosen, (((1,), (1,)), ((), ())), preferred_element_type=jnp.float32)
        source = source.astype(jnp.int32)
        for r in parts:
            sorted_ref[r:r + ROWS, at] = jnp.take_along_axis(total[r:r + ROWS], source, axis=1)
        return carry

    lax.fori_loop(0, blocks, reflect, 0, unroll=4)
    load_table.wait()

    def place_group(first, count):
        def step(j, held):
            values = [sorted_ref[r:r + ROWS, tile_at(j)] for r in parts]
            new = []
            for i in range(count):
                word = table_smem[first + i, j]
                low, keep, turn, at = low_of(word), keep_of(word), word & (LANES - 1), tile_at(tile_of(word))
                for n, r in enumerate(parts):
                    turned = pltpu.roll(values[n], turn, 1)
                    out = refs[1].at[first + i] if targets > DIRECT else outs[i]
                    out[r:r + ROWS, at] = jnp.where(lane >= low, turned, held[i * len(parts) + n])
                    new.append(jnp.where(lane >= keep, turned, held[i * len(parts) + n]))
            return tuple(new)

        zero = jnp.zeros((ROWS, LANES), jnp.float32)
        held = lax.fori_loop(0, blocks, step, (zero,) * (count * len(parts)), unroll=2)
        for i in range(count):
            out = refs[1].at[first + i] if targets > DIRECT else outs[i]
            word = table_smem[first + i, blocks]
            for n, r in enumerate(parts):
                out[r:r + ROWS, tile_at(tile_of(word))] = jnp.where(lane < low_of(word), held[i * len(parts) + n], 0.0)

    if targets <= GROUP:
        place_group(0, targets)
    else:
        @pl.loop(0, targets // GROUP)
        def _(g):
            place_group(g * GROUP, GROUP)


def pick_weights(w_ref, picked_ref, order, rows):
    gates = picked_ref.shape[-1]
    levels = picked_ref.shape[0] // len(order)
    for part in range(w_ref.shape[1] // gates):
        @pl.when(rows == part)
        def _():
            for i, l in enumerate(order):
                block = w_ref[pl.ds(pl.multiple_of(l * levels, levels), levels), :]
                picked_ref[i * levels:(i + 1) * levels, :] = block[:, part * gates:(part + 1) * gates]


def adjoint_kernel(targets, group, w_ref, own_ref, near_ref, *refs):
    out_refs, picked_ref = refs[:-1], refs[-1]
    levels, capacity = out_refs[0].shape[1:]
    me = first_target(targets)
    mine = lax.axis_index("lev")
    order = [mine ^ (2 * m) for m in range(len(out_refs))]
    for i in range(2):
        pick_weights(w_ref, picked_ref.at[i], order, mine ^ i)

    def step(s, carry):
        at = (group.start + group.step * s) ^ me
        at = pl.ds(pl.multiple_of(at * capacity, capacity), capacity)
        total = split_dot(picked_ref[0], own_ref[:, at]) + split_dot(picked_ref[1], near_ref[:, at])
        for i, out_ref in enumerate(out_refs):
            out_ref[s] = total[i * levels:(i + 1) * levels]
        return carry

    lax.fori_loop(0, len(group), step, 0)


def gate_part(targets, group, w_ref, sources, out_any, buffer, picked_ref, sem):
    mine = lax.axis_index("lev")
    half = len(sources) // 2
    order = [mine ^ (2 * (i % half)) ^ (i // half) for i in range(len(sources))]
    pick_weights(w_ref, picked_ref, order, mine)
    capacity = sources[0].shape[-1]
    me = first_target(targets)
    weights = picked_ref[...].T

    def column(s):
        return pl.ds(pl.multiple_of(((group.start + group.step * s) ^ me) * capacity, capacity), capacity)

    def store(s):
        part = pl.ds(pl.multiple_of(s * capacity, capacity), capacity)
        return pltpu.make_async_copy(buffer.at[:, part], out_any.at[:, column(s)], sem.at[s])

    def step(s, carry):
        part = pl.ds(pl.multiple_of(s * capacity, capacity), capacity)
        buffer[:, part] = split_dot(weights, jnp.concatenate([ref[s] for ref in sources], 0))
        store(s).start()
        return carry

    def finish(s, carry):
        store(s).wait()
        return carry

    lax.fori_loop(0, len(group), step, 0)
    return lambda: lax.fori_loop(0, len(group), finish, 0)


def increment_part(targets, table_ref, rank_ref, t_ref, slope_ref, refs, out_any, out_ref, sem):
    backs = blocks_of(refs)
    levels, _ = backs[0].shape
    blocks = rank_ref.shape[0]
    lane = iota((ROWS, LANES), 1)
    parts = range(0, levels, ROWS)
    me = first_target(targets)
    count = min(GROUP, targets)

    def block(j, carry):
        index = jnp.broadcast_to(rank_ref[pl.ds(j, 1), :] & (LANES - 1), (ROWS, LANES))
        target = jnp.broadcast_to(t_ref[pl.ds(j, 1), :], (ROWS, LANES)) ^ me

        def pick(first, found):
            found = list(found)
            for i in range(count):
                word = table_ref[first + i, j]
                low, tile, later = low_of(word), tile_of(word), lax.shift_right_logical(word, 28)
                back = refs[0].at[first + i] if targets > DIRECT else backs[i]
                for n, r in enumerate(parts):
                    window = jnp.where(lane >= low, back[r:r + ROWS, tile_at(tile)], back[r:r + ROWS, tile_at(later)])
                    moved = jnp.take_along_axis(window, index, axis=1)
                    found[n] = jnp.where(target == first + i, moved, found[n])
            return tuple(found)

        found = (jnp.zeros((ROWS, LANES), jnp.float32),) * len(parts)
        if targets <= count:
            found = pick(0, found)
        else:
            found = lax.fori_loop(0, targets // count, lambda g, f: pick(g * count, f), found)
        for k in range(3):
            for n, r in enumerate(parts):
                out_ref[k, r:r + ROWS, tile_at(j)] = slope_ref[k, r:r + ROWS, tile_at(j)] * found[n]
        return carry

    pieces = sem.shape[0]
    stores = []
    for p in range(pieces):
        first, last = blocks * p // pieces, blocks * (p + 1) // pieces
        if targets <= count:
            for j in range(first, last):
                block(j, 0)
        else:
            lax.fori_loop(first, last, block, 0, unroll=4)
        here = slice(first * LANES, last * LANES)
        stores.append(pltpu.make_async_copy(out_ref.at[:, :, here], out_any.at[:, :, here], sem.at[p]))
        stores[-1].start()
    return lambda: [store.wait() for store in stores]


def picked_sources(refs, picks):
    return [refs[operand] if at is None else refs[operand].at[at] for operand, at in picks]


def gate_kernel(targets, group, picks, w_ref, *refs):
    out_any, buffer, picked_ref, sem = refs[-4:]
    sources = picked_sources(refs, picks)
    gate_part(targets, group, w_ref, sources, out_any, buffer, picked_ref, sem)()


def final_kernel(targets, group, picks, columns, backs, table_ref, rank_ref, t_ref, slope_ref, w_ref, *refs):
    sources, refs = picked_sources(refs, picks), refs[columns:]
    returned, refs = refs[:backs], refs[backs:]
    gate_any, out_any, buffer, picked_ref, gate_sem, out_ref, out_sem = refs[-7:]
    gates_done = gate_part(targets, group, w_ref, sources, gate_any, buffer, picked_ref, gate_sem)
    increments_done = increment_part(
        targets, table_ref, rank_ref, t_ref, slope_ref, returned, out_any, out_ref, out_sem)
    gates_done()
    increments_done()


def settings(mib, micros):
    cost = pl.CostEstimate(flops=int(micros * 1e9), bytes_accessed=0, transcendentals=0)
    return dict(compiler_params=pltpu.CompilerParams(vmem_limit_bytes=mib << 20), cost_estimate=cost)


def full(space=pltpu.VMEM):
    return pl.BlockSpec(memory_space=space)


def per_device(mixing, density, routes, beam_weight, gate_adjoint):
    tile_count = lax.axis_size("tile")
    level_count = lax.axis_size("lev")
    level_dev, column_dev = density.shape
    capacity = 2 * column_dev // tile_count
    blocks = column_dev // LANES
    far = level_count // 2
    gate_dev = gate_adjoint.shape[0]
    direct = tile_count <= DIRECT
    f32, i32 = jnp.float32, jnp.int32
    shape = jax.ShapeDtypeStruct

    def swap(x, bits):
        return lax.ppermute(x, "lev", [(i, i ^ bits) for i in range(level_count)])

    def exchange(x, bits):
        return lax.ppermute(x, "tile", [(i, i ^ bits) for i in range(tile_count)])

    weights = beam_weight[0].T
    t = routes.reshape(blocks, LANES)
    table_shape = (max(tile_count, ROWS), LANES)
    half = tile_count // 2
    if direct:
        block_shapes = [shape((level_dev, capacity), f32)] * tile_count
        groups = [range(1, tile_count, 2), range(0, tile_count, 2)]
        sites = [range(0, tile_count, 2), range(1, tile_count, 2)]
    else:
        block_shapes = [shape((tile_count, level_dev, capacity), f32)]
        groups = sites = [range(0, tile_count)]

    near_adjoint = swap(gate_adjoint, 1)
    table, rank, place = pl.pallas_call(
        functools.partial(rank_kernel, tile_count, capacity // LANES),
        out_shape=[shape(table_shape, i32)] + [shape((blocks, LANES), i32)] * 2,
        in_specs=[full()],
        out_specs=[full()] * 3,
        **settings(12, 1),
    )(t)
    slopes, *outgoing = pl.pallas_call(
        functools.partial(source_kernel, tile_count),
        out_shape=[shape(mixing.shape, f32)] + block_shapes,
        in_specs=[full()] * 4,
        out_specs=[full()] * (1 + len(block_shapes)),
        scratch_shapes=[
            pltpu.VMEM(density.shape, f32),
            pltpu.SMEM(table_shape, i32),
            pltpu.SemaphoreType.DMA,
        ],
        **settings(12, 4),
    )(table, place, mixing, density)

    partial = []
    for group in groups:
        partial.append(pl.pallas_call(
            functools.partial(adjoint_kernel, tile_count, group),
            out_shape=[shape((len(group), level_dev, capacity), f32)] * far,
            in_specs=[full()] * 3,
            out_specs=[full()] * far,
            scratch_shapes=[pltpu.VMEM((2, far * level_dev, gate_dev), f32)],
            **settings(12, 2),
        )(weights, gate_adjoint, near_adjoint))

    totals = []
    for parts in partial:
        total = parts[0]
        for m in range(1, far):
            part = swap(parts[m], 2 * m)
            total = total + part
        totals.append(total)
    if direct:
        mixed = jnp.concatenate([lax.optimization_barrier(totals[0]), outgoing[1][None]], 0)
        crossed = exchange(lax.optimization_barrier(mixed), 1)
        incoming = [outgoing[0], crossed[half]]
        for k in range(2, tile_count):
            incoming.append(exchange(outgoing[k], k))
        arrived = []
        for site in sites:
            arrived.append(lax.optimization_barrier(jnp.stack([incoming[k] for k in site])))
        restored = []
        for p in range(half):
            pair = jnp.stack([totals[1][p], crossed[p]])
            restored.append(pair if p == 0 else exchange(pair, 2 * p))
    else:
        arrived = [lax.all_to_all(outgoing[0], "tile", split_axis=0, concat_axis=0, tiled=True)]
        restored = [lax.all_to_all(totals[0], "tile", split_axis=0, concat_axis=0, tiled=True)]

    passed = []
    for here in arrived:
        received = []
        for m in range(1, far):
            received.append(swap(here, 2 * m))
        passed.append(received)
    early = jnp.stack(arrived)
    early = swap(early, 1)
    beside = []
    for received in passed:
        beside.append([swap(x, 1) for x in received])

    gate_values = None
    for n, (group, here) in enumerate(zip(sites, arrived)):
        final = n + 1 == len(sites)
        columns = [here] + passed[n] + [early] + beside[n]
        picks = [(i, None) for i in range(far)] + [(far, n)] + [(far + m, None) for m in range(1, far)]
        before = [] if gate_values is None else [gate_values]
        gate_scratch = [
            pltpu.VMEM((gate_dev, len(group) * capacity), f32),
            pltpu.VMEM(weights.shape[:1] + (gate_dev,), f32),
            pltpu.SemaphoreType.DMA((len(group),)),
        ]
        if not final:
            gate_values = pl.pallas_call(
                functools.partial(gate_kernel, tile_count, group, picks),
                out_shape=shape(gate_adjoint.shape, f32),
                in_specs=[full()] * (1 + len(columns)) + [full(pltpu.HBM)] * len(before),
                out_specs=full(pltpu.HBM),
                input_output_aliases={1 + len(columns): 0} if before else {},
                scratch_shapes=gate_scratch,
                **settings(12, 2),
            )(weights, *columns, *before)
            continue
        operands = [table, rank, t, slopes, weights, *columns, *restored]
        gate_values, increments = pl.pallas_call(
            functools.partial(final_kernel, tile_count, group, picks, len(columns), len(restored)),
            out_shape=[shape(gate_adjoint.shape, f32), shape(mixing.shape, f32)],
            in_specs=[full(SMEM)] + [full()] * (len(operands) - 1) + [full(pltpu.HBM)] * len(before),
            out_specs=[full(pltpu.HBM)] * 2,
            input_output_aliases={len(operands): 0} if before else {},
            scratch_shapes=gate_scratch + [pltpu.VMEM(mixing.shape, f32), pltpu.SemaphoreType.DMA((4,))],
            **settings(16, 4),
        )(*operands, *before)
    return gate_values, increments


def solution(mesh):
    return jax.shard_map(
        per_device,
        mesh=mesh,
        in_specs=(
            P(None, "lev", "tile"),
            P("lev", "tile"),
            P("tile", None),
            P("tile", None, None),
            P("lev", "tile"),
        ),
        out_specs=(P("lev", "tile"), P(None, "lev", "tile")),
        check_vma=False,
    )
```

```python
import functools

import jax
import jax.numpy as jnp
from jax import lax
from jax.experimental import pallas as pl
from jax.experimental.pallas import tpu as pltpu
from jax.sharding import PartitionSpec as P

coefficients = (3.63, 0.96, 1.98)
exponents = (1.75, 1.66, 1.75)
LANES = 128
ROWS = 8
GROUP = 8
DIRECT = 8


def iota(shape, dim):
    return lax.broadcasted_iota(jnp.int32, shape, dim)


def tile_at(index):
    if isinstance(index, int):
        return slice(index * LANES, (index + 1) * LANES)
    return pl.ds(pl.multiple_of(index * LANES, LANES), LANES)


def halves(x):
    high = x.astype(jnp.bfloat16)
    low = (x - high.astype(jnp.float32)).astype(jnp.bfloat16)
    return high, low


def split_dot(weights, x):
    w_high, w_low = halves(weights)
    x_high, x_low = halves(x)
    rows = weights.shape[0]
    both = jnp.dot(jnp.concatenate([w_high, w_low], 0), x_high, preferred_element_type=jnp.float32)
    rest = jnp.dot(w_high, x_low, preferred_element_type=jnp.float32)
    return both[:rows] + (both[rows:] + rest)


def first_target(targets):
    return lax.axis_index("tile") if targets <= DIRECT else 0


def blocks_of(refs):
    return [ref.at[i] for ref in refs if len(ref.shape) == 3 for i in range(ref.shape[0])] or list(refs)


def tile_of(word):
    return (word >> 23) & 31


def low_of(word):
    return (jnp.full((ROWS, LANES), word, jnp.int32) >> 7) & 255


def keep_of(word):
    return (jnp.full((ROWS, LANES), word, jnp.int32) >> 15) & 255


def rank_kernel(targets, tiles, t_ref, table_ref, rank_ref, place_ref):
    t = t_ref[...]
    me = first_target(targets)
    blocks = t.shape[0]
    rows = blocks + ROWS
    before = (iota((LANES, LANES), 0) <= iota((LANES, LANES), 1)).astype(jnp.float32)
    sums = jnp.concatenate([before, jnp.ones((LANES, LANES), jnp.float32)], 1).astype(jnp.bfloat16)
    earlier = (iota((rows, blocks), 1) < iota((rows, blocks), 0)).astype(jnp.float32).astype(jnp.bfloat16)
    lane = iota((1, LANES), 1)
    start = jnp.zeros((blocks, LANES), jnp.float32)
    rank = jnp.zeros((blocks, LANES), jnp.float32)
    place = jnp.zeros((blocks, LANES), jnp.float32)
    starts = jnp.zeros((blocks, LANES), jnp.float32)
    numbers = jnp.zeros((blocks, LANES), jnp.float32)
    offsets = jnp.zeros((rows, LANES), jnp.float32)
    for first in range(0, targets, GROUP):
        group = range(first, min(first + GROUP, targets))
        masks = [t == d for d in group]
        ones = jnp.concatenate([m.astype(jnp.float32) for m in masks], 0).astype(jnp.bfloat16)
        counted = jnp.dot(ones, sums, preferred_element_type=jnp.float32)
        totals = [counted[i * blocks:(i + 1) * blocks, LANES:] for i in range(len(masks))]
        based = jnp.dot(earlier, jnp.concatenate(totals, 1).astype(jnp.bfloat16), preferred_element_type=jnp.float32)
        for i, d in enumerate(group):
            inclusive = counted[i * blocks:(i + 1) * blocks, :LANES]
            base = based[:, i * LANES:(i + 1) * LANES]
            mine = lane % targets == d ^ me
            rank = jnp.where(masks[i], base[:blocks] + inclusive - 1.0, rank)
            place = jnp.where(masks[i], start + inclusive - 1.0, place)
            starts = jnp.where(mine, start, starts)
            numbers = jnp.where(mine, totals[i], numbers)
            offsets = jnp.where(mine, base, offsets)
            start = start + totals[i]
    pad = jnp.zeros((rows - blocks, LANES), jnp.int32)
    starts = jnp.concatenate([starts.astype(jnp.int32), pad], 0)
    numbers = jnp.concatenate([numbers.astype(jnp.int32), pad], 0)
    offsets = offsets.astype(jnp.int32)
    tile = jnp.minimum(offsets >> 7, tiles - 1)
    low = jnp.where(offsets == tiles * LANES, LANES, offsets & (LANES - 1))
    keep = jnp.where((low + numbers >= LANES) & (tile + 1 < tiles), 0, low)
    turn = (low - starts) & (LANES - 1)
    later = jnp.minimum(tile + 1, tiles - 1)
    word = turn | (low << 7) | (keep << 15) | (tile << 23) | (later << 28)
    word = jnp.concatenate([word, jnp.zeros((LANES - rows, LANES), jnp.int32)], 0)
    table_ref[...] = word.T[:table_ref.shape[0]]
    rank_ref[...] = rank.astype(jnp.int32)
    place_ref[...] = place.astype(jnp.int32)


def source_kernel(targets, table_ref, place_ref, mixing_ref, density_ref, *refs):
    slope_ref, outs = refs[0], blocks_of(refs[1:-3])
    sorted_ref, table_smem, table_sem = refs[-3:]
    levels, capacity = outs[0].shape
    blocks = place_ref.shape[0]
    load_table = pltpu.make_async_copy(table_ref, table_smem, table_sem)
    load_table.start()
    lanes_row = iota((ROWS, LANES), 1).astype(jnp.float32).astype(jnp.bfloat16)
    sublane = iota((LANES, LANES), 0)
    lane = iota((ROWS, LANES), 1)
    parts = range(0, levels, ROWS)
    for out in outs:
        out[...] = jnp.zeros((levels, capacity), jnp.float32)

    def reflect(j, carry):
        at = tile_at(j)
        rho = density_ref[:, at]
        total = jnp.zeros((levels, LANES), jnp.float32)
        for k in range(3):
            q = mixing_ref[k, :, at]
            powered = coefficients[k] * jnp.exp(exponents[k] * jnp.log(rho * q))
            total = total + powered
            slope_ref[k, :, at] = exponents[k] * powered / q
        chosen = (sublane == place_ref[pl.ds(j, 1), :]).astype(jnp.float32).astype(jnp.bfloat16)
        source = lax.dot_general(lanes_row, chosen, (((1,), (1,)), ((), ())), preferred_element_type=jnp.float32)
        source = source.astype(jnp.int32)
        for r in parts:
            sorted_ref[r:r + ROWS, at] = jnp.take_along_axis(total[r:r + ROWS], source, axis=1)
        return carry

    lax.fori_loop(0, blocks, reflect, 0, unroll=4)
    load_table.wait()

    def place_group(first, count):
        def step(j, held):
            values = [sorted_ref[r:r + ROWS, tile_at(j)] for r in parts]
            new = []
            for i in range(count):
                word = table_smem[first + i, j]
                low, keep, turn, at = low_of(word), keep_of(word), word & (LANES - 1), tile_at(tile_of(word))
                for n, r in enumerate(parts):
                    turned = pltpu.roll(values[n], turn, 1)
                    out = refs[1].at[first + i] if targets > DIRECT else outs[i]
                    out[r:r + ROWS, at] = jnp.where(lane >= low, turned, held[i * len(parts) + n])
                    new.append(jnp.where(lane >= keep, turned, held[i * len(parts) + n]))
            return tuple(new)

        zero = jnp.zeros((ROWS, LANES), jnp.float32)
        held = lax.fori_loop(0, blocks, step, (zero,) * (count * len(parts)), unroll=2)
        for i in range(count):
            out = refs[1].at[first + i] if targets > DIRECT else outs[i]
            word = table_smem[first + i, blocks]
            for n, r in enumerate(parts):
                out[r:r + ROWS, tile_at(tile_of(word))] = jnp.where(lane < low_of(word), held[i * len(parts) + n], 0.0)

    if targets <= GROUP:
        place_group(0, targets)
    else:
        @pl.loop(0, targets // GROUP)
        def _(g):
            place_group(g * GROUP, GROUP)


def pick_weights(w_ref, picked_ref, order, rows):
    gates = picked_ref.shape[-1]
    levels = picked_ref.shape[0] // len(order)
    for part in range(w_ref.shape[1] // gates):
        @pl.when(rows == part)
        def _():
            for i, l in enumerate(order):
                block = w_ref[pl.ds(pl.multiple_of(l * levels, levels), levels), :]
                picked_ref[i * levels:(i + 1) * levels, :] = block[:, part * gates:(part + 1) * gates]


def adjoint_kernel(targets, group, w_ref, own_ref, near_ref, *refs):
    out_refs, picked_ref = refs[:-1], refs[-1]
    levels, capacity = out_refs[0].shape[1:]
    me = first_target(targets)
    mine = lax.axis_index("lev")
    order = [mine ^ (2 * m) for m in range(len(out_refs))]
    for i in range(2):
        pick_weights(w_ref, picked_ref.at[i], order, mine ^ i)

    def step(s, carry):
        at = (group.start + group.step * s) ^ me
        at = pl.ds(pl.multiple_of(at * capacity, capacity), capacity)
        total = split_dot(picked_ref[0], own_ref[:, at]) + split_dot(picked_ref[1], near_ref[:, at])
        for i, out_ref in enumerate(out_refs):
            out_ref[s] = total[i * levels:(i + 1) * levels]
        return carry

    lax.fori_loop(0, len(group), step, 0)


def gate_part(targets, group, w_ref, sources, out_any, buffer, picked_ref, sem):
    mine = lax.axis_index("lev")
    half = len(sources) // 2
    order = [mine ^ (2 * (i % half)) ^ (i // half) for i in range(len(sources))]
    pick_weights(w_ref, picked_ref, order, mine)
    capacity = sources[0].shape[-1]
    me = first_target(targets)
    weights = picked_ref[...].T

    def column(s):
        return pl.ds(pl.multiple_of(((group.start + group.step * s) ^ me) * capacity, capacity), capacity)

    def store(s):
        part = pl.ds(pl.multiple_of(s * capacity, capacity), capacity)
        return pltpu.make_async_copy(buffer.at[:, part], out_any.at[:, column(s)], sem.at[s])

    def step(s, carry):
        part = pl.ds(pl.multiple_of(s * capacity, capacity), capacity)
        buffer[:, part] = split_dot(weights, jnp.concatenate([ref[s] for ref in sources], 0))
        store(s).start()
        return carry

    def finish(s, carry):
        store(s).wait()
        return carry

    lax.fori_loop(0, len(group), step, 0)
    return lambda: lax.fori_loop(0, len(group), finish, 0)


def increment_kernel(targets, table_ref, rank_ref, t_ref, slope_ref, *refs):
    refs, out_ref = refs[:-1], refs[-1]
    backs = blocks_of(refs)
    levels, _ = backs[0].shape
    blocks = rank_ref.shape[0]
    lane = iota((ROWS, LANES), 1)
    parts = range(0, levels, ROWS)
    me = first_target(targets)
    count = min(GROUP, targets)

    def block(j, carry):
        index = jnp.broadcast_to(rank_ref[pl.ds(j, 1), :] & (LANES - 1), (ROWS, LANES))
        target = jnp.broadcast_to(t_ref[pl.ds(j, 1), :], (ROWS, LANES)) ^ me

        def pick(first, found):
            found = list(found)
            for i in range(count):
                word = table_ref[first + i, j]
                low, tile, later = low_of(word), tile_of(word), lax.shift_right_logical(word, 28)
                back = refs[0].at[first + i] if targets > DIRECT else backs[i]
                for n, r in enumerate(parts):
                    window = jnp.where(lane >= low, back[r:r + ROWS, tile_at(tile)], back[r:r + ROWS, tile_at(later)])
                    moved = jnp.take_along_axis(window, index, axis=1)
                    found[n] = jnp.where(target == first + i, moved, found[n])
            return tuple(found)

        found = (jnp.zeros((ROWS, LANES), jnp.float32),) * len(parts)
        if targets <= count:
            found = pick(0, found)
        else:
            found = lax.fori_loop(0, targets // count, lambda g, f: pick(g * count, f), found)
        for k in range(3):
            for n, r in enumerate(parts):
                out_ref[k, r:r + ROWS, tile_at(j)] = slope_ref[k, r:r + ROWS, tile_at(j)] * found[n]
        return carry

    if targets <= count:
        for j in range(blocks):
            block(j, 0)
    else:
        lax.fori_loop(0, blocks, block, 0, unroll=4)


def picked_sources(refs, picks):
    return [refs[operand] if at is None else refs[operand].at[at] for operand, at in picks]


def gate_kernel(targets, group, picks, w_ref, *refs):
    out_any, buffer, picked_ref, sem = refs[-4:]
    sources = picked_sources(refs, picks)
    gate_part(targets, group, w_ref, sources, out_any, buffer, picked_ref, sem)()


def final_kernel(targets, group, picks, columns, increment_ref, w_ref, *refs):
    sources = picked_sources(refs[:columns], picks)
    gate_any, out_any, buffer, picked_ref, gate_sem, out_sem = refs[-6:]
    store = pltpu.make_async_copy(increment_ref, out_any, out_sem)
    store.start()
    gate_part(targets, group, w_ref, sources, gate_any, buffer, picked_ref, gate_sem)()
    store.wait()


def settings(mib, micros):
    cost = pl.CostEstimate(flops=int(micros * 1e9), bytes_accessed=0, transcendentals=0)
    return dict(compiler_params=pltpu.CompilerParams(vmem_limit_bytes=mib << 20), cost_estimate=cost)


def full(space=pltpu.VMEM):
    return pl.BlockSpec(memory_space=space)


def per_device(mixing, density, routes, beam_weight, gate_adjoint):
    tile_count = lax.axis_size("tile")
    level_count = lax.axis_size("lev")
    level_dev, column_dev = density.shape
    capacity = 2 * column_dev // tile_count
    blocks = column_dev // LANES
    far = level_count // 2
    gate_dev = gate_adjoint.shape[0]
    direct = tile_count <= DIRECT
    f32, i32 = jnp.float32, jnp.int32
    shape = jax.ShapeDtypeStruct

    def swap(x, bits):
        return lax.ppermute(x, "lev", [(i, i ^ bits) for i in range(level_count)])

    def exchange(x, bits):
        return lax.ppermute(x, "tile", [(i, i ^ bits) for i in range(tile_count)])

    weights = beam_weight[0].T
    t = routes.reshape(blocks, LANES)
    table_shape = (max(tile_count, ROWS), LANES)
    half = tile_count // 2
    if direct:
        block_shapes = [shape((level_dev, capacity), f32)] * tile_count
        groups = [range(1, tile_count, 2), range(0, tile_count, 2)]
        sites = [range(0, tile_count, 2), range(1, tile_count, 2)]
    else:
        block_shapes = [shape((tile_count, level_dev, capacity), f32)]
        groups = sites = [range(0, tile_count)]

    near_adjoint = swap(gate_adjoint, 1)
    table, rank, place = pl.pallas_call(
        functools.partial(rank_kernel, tile_count, capacity // LANES),
        out_shape=[shape(table_shape, i32)] + [shape((blocks, LANES), i32)] * 2,
        in_specs=[full()],
        out_specs=[full()] * 3,
        **settings(12, 1),
    )(t)
    slopes, *outgoing = pl.pallas_call(
        functools.partial(source_kernel, tile_count),
        out_shape=[shape(mixing.shape, f32)] + block_shapes,
        in_specs=[full()] * 4,
        out_specs=[full()] * (1 + len(block_shapes)),
        scratch_shapes=[
            pltpu.VMEM(density.shape, f32),
            pltpu.SMEM(table_shape, i32),
            pltpu.SemaphoreType.DMA,
        ],
        **settings(12, 4),
    )(table, place, mixing, density)

    partial = []
    for group in groups:
        partial.append(pl.pallas_call(
            functools.partial(adjoint_kernel, tile_count, group),
            out_shape=[shape((len(group), level_dev, capacity), f32)] * far,
            in_specs=[full()] * 3,
            out_specs=[full()] * far,
            scratch_shapes=[pltpu.VMEM((2, far * level_dev, gate_dev), f32)],
            **settings(12, 2),
        )(weights, gate_adjoint, near_adjoint))

    totals = []
    for parts in partial:
        total = parts[0]
        for m in range(1, far):
            part = swap(parts[m], 2 * m)
            total = total + part
        totals.append(total)
    if direct:
        mixed = jnp.concatenate([lax.optimization_barrier(totals[0]), outgoing[1][None]], 0)
        crossed = exchange(lax.optimization_barrier(mixed), 1)
        incoming = [outgoing[0], crossed[half]]
        for k in range(2, tile_count):
            incoming.append(exchange(outgoing[k], k))
        arrived = []
        for site in sites:
            arrived.append(lax.optimization_barrier(jnp.stack([incoming[k] for k in site])))
        restored = []
        for p in range(half):
            pair = jnp.stack([totals[1][p], crossed[p]])
            restored.append(pair if p == 0 else exchange(pair, 2 * p))
    else:
        arrived = [lax.all_to_all(outgoing[0], "tile", split_axis=0, concat_axis=0, tiled=True)]
        restored = [lax.all_to_all(totals[0], "tile", split_axis=0, concat_axis=0, tiled=True)]

    passed = []
    for here in arrived:
        received = []
        for m in range(1, far):
            received.append(swap(here, 2 * m))
        passed.append(received)
    beside = []
    for n, received in enumerate(passed[:-1]):
        beside.append([swap(arrived[n], 1)])
        beside[n] += [swap(x, 1) for x in received]
    late = jnp.stack([arrived[-1]] + passed[-1])
    beside.append([swap(late, 1)])

    gate_values = None
    for n, (group, here) in enumerate(zip(sites, arrived)):
        final = n + 1 == len(sites)
        columns = [here] + passed[n] + beside[n]
        picks = [(i, None) for i in range(far)]
        picks += [(far, m) if final else (far + m, None) for m in range(far)]
        before = [] if gate_values is None else [gate_values]
        gate_scratch = [
            pltpu.VMEM((gate_dev, len(group) * capacity), f32),
            pltpu.VMEM(weights.shape[:1] + (gate_dev,), f32),
            pltpu.SemaphoreType.DMA((len(group),)),
        ]
        if not final:
            gate_values = pl.pallas_call(
                functools.partial(gate_kernel, tile_count, group, picks),
                out_shape=shape(gate_adjoint.shape, f32),
                in_specs=[full()] * (1 + len(columns)) + [full(pltpu.HBM)] * len(before),
                out_specs=full(pltpu.HBM),
                input_output_aliases={1 + len(columns): 0} if before else {},
                scratch_shapes=gate_scratch,
                **settings(12, 2),
            )(weights, *columns, *before)
            continue
        found = pl.pallas_call(
            functools.partial(increment_kernel, tile_count),
            out_shape=shape(mixing.shape, f32),
            in_specs=[full(pltpu.SMEM)] + [full()] * (3 + len(restored)),
            out_specs=full(),
            **settings(12, 1),
        )(table, rank, t, slopes, *restored)
        operands = [found, weights, *columns]
        gate_values, increments = pl.pallas_call(
            functools.partial(final_kernel, tile_count, group, picks, len(columns)),
            out_shape=[shape(gate_adjoint.shape, f32), shape(mixing.shape, f32)],
            in_specs=[full()] * len(operands) + [full(pltpu.HBM)] * len(before),
            out_specs=[full(pltpu.HBM)] * 2,
            input_output_aliases={len(operands): 0} if before else {},
            scratch_shapes=gate_scratch + [pltpu.SemaphoreType.DMA],
            **settings(16, 2),
        )(*operands, *before)
    return gate_values, increments


def solution(mesh):
    return jax.shard_map(
        per_device,
        mesh=mesh,
        in_specs=(
            P(None, "lev", "tile"),
            P("lev", "tile"),
            P("tile", None),
            P("tile", None, None),
            P("lev", "tile"),
        ),
        out_specs=(P("lev", "tile"), P(None, "lev", "tile")),
        check_vma=False,
    )
```

```python
import functools

import jax
import jax.numpy as jnp
from jax import lax
from jax.experimental import pallas as pl
from jax.experimental.pallas import tpu as pltpu
from jax.sharding import PartitionSpec as P

coefficients = (3.63, 0.96, 1.98)
exponents = (1.75, 1.66, 1.75)
LANES = 128
ROWS = 8
GROUP = 8
DIRECT = 8


def iota(shape, dim):
    return lax.broadcasted_iota(jnp.int32, shape, dim)


def tile_at(index):
    if isinstance(index, int):
        return slice(index * LANES, (index + 1) * LANES)
    return pl.ds(pl.multiple_of(index * LANES, LANES), LANES)


def halves(x):
    high = x.astype(jnp.bfloat16)
    low = (x - high.astype(jnp.float32)).astype(jnp.bfloat16)
    return high, low


def split_dot(weights, x):
    w_high, w_low = halves(weights)
    x_high, x_low = halves(x)
    rows = weights.shape[0]
    both = jnp.dot(jnp.concatenate([w_high, w_low], 0), x_high, preferred_element_type=jnp.float32)
    rest = jnp.dot(w_high, x_low, preferred_element_type=jnp.float32)
    return both[:rows] + (both[rows:] + rest)


def first_target(targets):
    return lax.axis_index("tile") if targets <= DIRECT else 0


def blocks_of(refs):
    return [ref.at[i] for ref in refs if len(ref.shape) == 3 for i in range(ref.shape[0])] or list(refs)


def tile_of(word):
    return (word >> 23) & 31


def low_of(word):
    return (jnp.full((ROWS, LANES), word, jnp.int32) >> 7) & 255


def keep_of(word):
    return (jnp.full((ROWS, LANES), word, jnp.int32) >> 15) & 255


def rank_kernel(targets, tiles, t_ref, table_ref, rank_ref, place_ref):
    t = t_ref[...]
    me = first_target(targets)
    blocks = t.shape[0]
    rows = blocks + ROWS
    before = (iota((LANES, LANES), 0) <= iota((LANES, LANES), 1)).astype(jnp.float32)
    sums = jnp.concatenate([before, jnp.ones((LANES, LANES), jnp.float32)], 1).astype(jnp.bfloat16)
    earlier = (iota((rows, blocks), 1) < iota((rows, blocks), 0)).astype(jnp.float32).astype(jnp.bfloat16)
    lane = iota((1, LANES), 1)
    start = jnp.zeros((blocks, LANES), jnp.float32)
    rank = jnp.zeros((blocks, LANES), jnp.float32)
    place = jnp.zeros((blocks, LANES), jnp.float32)
    starts = jnp.zeros((blocks, LANES), jnp.float32)
    numbers = jnp.zeros((blocks, LANES), jnp.float32)
    offsets = jnp.zeros((rows, LANES), jnp.float32)
    for first in range(0, targets, GROUP):
        group = range(first, min(first + GROUP, targets))
        masks = [t == d for d in group]
        ones = jnp.concatenate([m.astype(jnp.float32) for m in masks], 0).astype(jnp.bfloat16)
        counted = jnp.dot(ones, sums, preferred_element_type=jnp.float32)
        totals = [counted[i * blocks:(i + 1) * blocks, LANES:] for i in range(len(masks))]
        based = jnp.dot(earlier, jnp.concatenate(totals, 1).astype(jnp.bfloat16), preferred_element_type=jnp.float32)
        for i, d in enumerate(group):
            inclusive = counted[i * blocks:(i + 1) * blocks, :LANES]
            base = based[:, i * LANES:(i + 1) * LANES]
            mine = lane % targets == d ^ me
            rank = jnp.where(masks[i], base[:blocks] + inclusive - 1.0, rank)
            place = jnp.where(masks[i], start + inclusive - 1.0, place)
            starts = jnp.where(mine, start, starts)
            numbers = jnp.where(mine, totals[i], numbers)
            offsets = jnp.where(mine, base, offsets)
            start = start + totals[i]
    pad = jnp.zeros((rows - blocks, LANES), jnp.int32)
    starts = jnp.concatenate([starts.astype(jnp.int32), pad], 0)
    numbers = jnp.concatenate([numbers.astype(jnp.int32), pad], 0)
    offsets = offsets.astype(jnp.int32)
    tile = jnp.minimum(offsets >> 7, tiles - 1)
    low = jnp.where(offsets == tiles * LANES, LANES, offsets & (LANES - 1))
    keep = jnp.where((low + numbers >= LANES) & (tile + 1 < tiles), 0, low)
    turn = (low - starts) & (LANES - 1)
    later = jnp.minimum(tile + 1, tiles - 1)
    word = turn | (low << 7) | (keep << 15) | (tile << 23) | (later << 28)
    word = jnp.concatenate([word, jnp.zeros((LANES - rows, LANES), jnp.int32)], 0)
    table_ref[...] = word.T[:table_ref.shape[0]]
    rank_ref[...] = rank.astype(jnp.int32)
    place_ref[...] = place.astype(jnp.int32)


def source_kernel(targets, table_ref, place_ref, mixing_ref, density_ref, *refs):
    slope_ref, outs = refs[0], blocks_of(refs[1:-3])
    sorted_ref, table_smem, table_sem = refs[-3:]
    levels, capacity = outs[0].shape
    blocks = place_ref.shape[0]
    load_table = pltpu.make_async_copy(table_ref, table_smem, table_sem)
    load_table.start()
    lanes_row = iota((ROWS, LANES), 1).astype(jnp.float32).astype(jnp.bfloat16)
    sublane = iota((LANES, LANES), 0)
    lane = iota((ROWS, LANES), 1)
    parts = range(0, levels, ROWS)
    for out in outs:
        out[...] = jnp.zeros((levels, capacity), jnp.float32)

    def reflect(j, carry):
        at = tile_at(j)
        rho = density_ref[:, at]
        total = jnp.zeros((levels, LANES), jnp.float32)
        for k in range(3):
            q = mixing_ref[k, :, at]
            powered = coefficients[k] * jnp.exp(exponents[k] * jnp.log(rho * q))
            total = total + powered
            slope_ref[k, :, at] = exponents[k] * powered / q
        chosen = (sublane == place_ref[pl.ds(j, 1), :]).astype(jnp.float32).astype(jnp.bfloat16)
        source = lax.dot_general(lanes_row, chosen, (((1,), (1,)), ((), ())), preferred_element_type=jnp.float32)
        source = source.astype(jnp.int32)
        for r in parts:
            sorted_ref[r:r + ROWS, at] = jnp.take_along_axis(total[r:r + ROWS], source, axis=1)
        return carry

    lax.fori_loop(0, blocks, reflect, 0, unroll=4)
    load_table.wait()

    def place_group(first, count):
        def step(j, held):
            values = [sorted_ref[r:r + ROWS, tile_at(j)] for r in parts]
            new = []
            for i in range(count):
                word = table_smem[first + i, j]
                low, keep, turn, at = low_of(word), keep_of(word), word & (LANES - 1), tile_at(tile_of(word))
                for n, r in enumerate(parts):
                    turned = pltpu.roll(values[n], turn, 1)
                    out = refs[1].at[first + i] if targets > DIRECT else outs[i]
                    out[r:r + ROWS, at] = jnp.where(lane >= low, turned, held[i * len(parts) + n])
                    new.append(jnp.where(lane >= keep, turned, held[i * len(parts) + n]))
            return tuple(new)

        zero = jnp.zeros((ROWS, LANES), jnp.float32)
        held = lax.fori_loop(0, blocks, step, (zero,) * (count * len(parts)), unroll=2)
        for i in range(count):
            out = refs[1].at[first + i] if targets > DIRECT else outs[i]
            word = table_smem[first + i, blocks]
            for n, r in enumerate(parts):
                out[r:r + ROWS, tile_at(tile_of(word))] = jnp.where(lane < low_of(word), held[i * len(parts) + n], 0.0)

    if targets <= GROUP:
        place_group(0, targets)
    else:
        @pl.loop(0, targets // GROUP)
        def _(g):
            place_group(g * GROUP, GROUP)


def pick_weights(w_ref, picked_ref, order, rows):
    gates = picked_ref.shape[-1]
    levels = picked_ref.shape[0] // len(order)
    for part in range(w_ref.shape[1] // gates):
        @pl.when(rows == part)
        def _():
            for i, l in enumerate(order):
                block = w_ref[pl.ds(pl.multiple_of(l * levels, levels), levels), :]
                picked_ref[i * levels:(i + 1) * levels, :] = block[:, part * gates:(part + 1) * gates]


def adjoint_kernel(targets, group, w_ref, own_ref, near_ref, *refs):
    out_refs, picked_ref = refs[:-1], refs[-1]
    levels, capacity = out_refs[0].shape[1:]
    me = first_target(targets)
    mine = lax.axis_index("lev")
    order = [mine ^ (2 * m) for m in range(len(out_refs))]
    for i in range(2):
        pick_weights(w_ref, picked_ref.at[i], order, mine ^ i)

    def step(s, carry):
        at = (group.start + group.step * s) ^ me
        at = pl.ds(pl.multiple_of(at * capacity, capacity), capacity)
        total = split_dot(picked_ref[0], own_ref[:, at]) + split_dot(picked_ref[1], near_ref[:, at])
        for i, out_ref in enumerate(out_refs):
            out_ref[s] = total[i * levels:(i + 1) * levels]
        return carry

    lax.fori_loop(0, len(group), step, 0, unroll=2)


def gate_part(targets, group, w_ref, sources, out_any, buffer, picked_ref, sem):
    mine = lax.axis_index("lev")
    half = len(sources) // 2
    order = [mine ^ (2 * (i % half)) ^ (i // half) for i in range(len(sources))]
    pick_weights(w_ref, picked_ref, order, mine)
    capacity = sources[0].shape[-1]
    weights = picked_ref[...].T

    def step(s, carry):
        part = pl.ds(pl.multiple_of(s * capacity, capacity), capacity)
        buffer[:, part] = split_dot(weights, jnp.concatenate([ref[s] for ref in sources], 0))
        if out_any is not None:
            gate_store(targets, group, capacity, out_any, buffer, sem, s).start()
        return carry

    lax.fori_loop(0, len(group), step, 0, unroll=2)


def gate_store(targets, group, capacity, out_any, buffer, sem, s):
    at = (group.start + group.step * s) ^ first_target(targets)
    column = pl.ds(pl.multiple_of(at * capacity, capacity), capacity)
    part = pl.ds(pl.multiple_of(s * capacity, capacity), capacity)
    return pltpu.make_async_copy(buffer.at[:, part], out_any.at[:, column], sem.at[s])


def increment_kernel(targets, table_ref, rank_ref, t_ref, slope_ref, *refs):
    refs, out_ref = refs[:-1], refs[-1]
    backs = blocks_of(refs)
    levels, _ = backs[0].shape
    blocks = rank_ref.shape[0]
    lane = iota((ROWS, LANES), 1)
    parts = range(0, levels, ROWS)
    me = first_target(targets)
    count = min(GROUP, targets)

    def block(j, carry):
        index = jnp.broadcast_to(rank_ref[pl.ds(j, 1), :] & (LANES - 1), (ROWS, LANES))
        target = jnp.broadcast_to(t_ref[pl.ds(j, 1), :], (ROWS, LANES)) ^ me

        def pick(first, found):
            found = list(found)
            for i in range(count):
                word = table_ref[first + i, j]
                low, tile, later = low_of(word), tile_of(word), lax.shift_right_logical(word, 28)
                back = refs[0].at[first + i] if targets > DIRECT else backs[i]
                for n, r in enumerate(parts):
                    window = jnp.where(lane >= low, back[r:r + ROWS, tile_at(tile)], back[r:r + ROWS, tile_at(later)])
                    moved = jnp.take_along_axis(window, index, axis=1)
                    found[n] = jnp.where(target == first + i, moved, found[n])
            return tuple(found)

        found = (jnp.zeros((ROWS, LANES), jnp.float32),) * len(parts)
        if targets <= count:
            found = pick(0, found)
        else:
            found = lax.fori_loop(0, targets // count, lambda g, f: pick(g * count, f), found)
        for k in range(3):
            for n, r in enumerate(parts):
                out_ref[k, r:r + ROWS, tile_at(j)] = slope_ref[k, r:r + ROWS, tile_at(j)] * found[n]
        return carry

    if targets <= count:
        for j in range(blocks):
            block(j, 0)
    else:
        lax.fori_loop(0, blocks, block, 0, unroll=4)


def picked_sources(refs, picks):
    return [refs[operand] if at is None else refs[operand].at[at] for operand, at in picks]


def gate_kernel(targets, group, picks, w_ref, *refs):
    buffer, picked_ref = refs[-2:]
    gate_part(targets, group, w_ref, picked_sources(refs[:-2], picks), None, buffer, picked_ref, None)


def final_kernel(targets, groups, picks, columns, increment_ref, w_ref, *refs):
    sources = picked_sources(refs[:columns], picks)
    gate_any, out_any, buffer, picked_ref, out_sem, *sems = refs[columns + len(groups) - 1:]
    buffers = [*refs[columns:columns + len(groups) - 1], buffer]
    capacity = sources[0].shape[-1]
    store = pltpu.make_async_copy(increment_ref, out_any, out_sem)
    store.start()
    stores = [
        [gate_store(targets, group, capacity, gate_any, held, sem, s) for s in range(len(group))]
        for group, held, sem in zip(groups, buffers, sems)
    ]
    for copies in stores[:-1]:
        for copy in copies:
            copy.start()
    gate_part(targets, groups[-1], w_ref, sources, gate_any, buffer, picked_ref, sems[-1])
    for copies in stores:
        for copy in copies:
            copy.wait()
    store.wait()


def settings(mib, micros):
    cost = pl.CostEstimate(flops=int(micros * 1e9), bytes_accessed=0, transcendentals=0)
    return dict(compiler_params=pltpu.CompilerParams(vmem_limit_bytes=mib << 20), cost_estimate=cost)


def full(space=pltpu.VMEM):
    return pl.BlockSpec(memory_space=space)


def per_device(mixing, density, routes, beam_weight, gate_adjoint):
    tile_count = lax.axis_size("tile")
    level_count = lax.axis_size("lev")
    level_dev, column_dev = density.shape
    capacity = 2 * column_dev // tile_count
    blocks = column_dev // LANES
    far = level_count // 2
    gate_dev = gate_adjoint.shape[0]
    direct = tile_count <= DIRECT
    f32, i32 = jnp.float32, jnp.int32
    shape = jax.ShapeDtypeStruct

    def swap(x, bits):
        return lax.ppermute(x, "lev", [(i, i ^ bits) for i in range(level_count)])

    def exchange(x, bits):
        return lax.ppermute(x, "tile", [(i, i ^ bits) for i in range(tile_count)])

    weights = beam_weight[0].T
    t = routes.reshape(blocks, LANES)
    table_shape = (max(tile_count, ROWS), LANES)
    half = tile_count // 2
    if direct:
        block_shapes = [shape((level_dev, capacity), f32)] * tile_count
        groups = [range(1, tile_count, 2), range(0, tile_count, 2)]
        sites = [range(0, tile_count, 2), range(1, tile_count, 2)]
    else:
        block_shapes = [shape((tile_count, level_dev, capacity), f32)]
        groups = sites = [range(0, tile_count)]

    near_adjoint = swap(gate_adjoint, 1)
    table, rank, place = pl.pallas_call(
        functools.partial(rank_kernel, tile_count, capacity // LANES),
        out_shape=[shape(table_shape, i32)] + [shape((blocks, LANES), i32)] * 2,
        in_specs=[full()],
        out_specs=[full()] * 3,
        **settings(12, 1),
    )(t)
    slopes, *outgoing = pl.pallas_call(
        functools.partial(source_kernel, tile_count),
        out_shape=[shape(mixing.shape, f32)] + block_shapes,
        in_specs=[full()] * 4,
        out_specs=[full()] * (1 + len(block_shapes)),
        scratch_shapes=[
            pltpu.VMEM(density.shape, f32),
            pltpu.SMEM(table_shape, i32),
            pltpu.SemaphoreType.DMA,
        ],
        **settings(12, 4),
    )(table, place, mixing, density)

    partial = []
    for group in groups:
        partial.append(pl.pallas_call(
            functools.partial(adjoint_kernel, tile_count, group),
            out_shape=[shape((len(group), level_dev, capacity), f32)] * far,
            in_specs=[full()] * 3,
            out_specs=[full()] * far,
            scratch_shapes=[pltpu.VMEM((2, far * level_dev, gate_dev), f32)],
            **settings(12, 2),
        )(weights, gate_adjoint, near_adjoint))

    totals = []
    for parts in partial:
        total = parts[0]
        for m in range(1, far):
            part = swap(parts[m], 2 * m)
            total = total + part
        totals.append(total)
    if direct:
        mixed = jnp.concatenate([lax.optimization_barrier(totals[0]), outgoing[1][None]], 0)
        crossed = exchange(lax.optimization_barrier(mixed), 1)
        incoming = [outgoing[0], crossed[half]]
        for k in range(2, tile_count):
            incoming.append(exchange(outgoing[k], k))
        arrived = []
        for site in sites:
            arrived.append(lax.optimization_barrier(jnp.stack([incoming[k] for k in site])))
        restored = []
        for p in range(half):
            pair = jnp.stack([totals[1][p], crossed[p]])
            restored.append(pair if p == 0 else exchange(pair, 2 * p))
    else:
        arrived = [lax.all_to_all(outgoing[0], "tile", split_axis=0, concat_axis=0, tiled=True)]
        restored = [lax.all_to_all(totals[0], "tile", split_axis=0, concat_axis=0, tiled=True)]

    passed = []
    for here in arrived:
        received = []
        for m in range(1, far):
            received.append(swap(here, 2 * m))
        passed.append(received)
    beside = []
    for n, received in enumerate(passed[:-1]):
        beside.append([swap(arrived[n], 1)])
        beside[n] += [swap(x, 1) for x in received]
    late = jnp.stack([arrived[-1]] + passed[-1])
    beside.append([swap(late, 1)])

    gates = []
    for n, (group, here) in enumerate(zip(sites, arrived)):
        final = n + 1 == len(sites)
        columns = [here] + passed[n] + beside[n]
        picks = [(i, None) for i in range(far)]
        picks += [(far, m) if final else (far + m, None) for m in range(far)]
        picked = pltpu.VMEM(weights.shape[:1] + (gate_dev,), f32)
        if not final:
            gates.append(pl.pallas_call(
                functools.partial(gate_kernel, tile_count, group, picks),
                out_shape=shape((gate_dev, len(group) * capacity), f32),
                in_specs=[full()] * (1 + len(columns)),
                out_specs=full(),
                scratch_shapes=[picked],
                **settings(12, 2),
            )(weights, *columns))
            continue
        found = pl.pallas_call(
            functools.partial(increment_kernel, tile_count),
            out_shape=shape(mixing.shape, f32),
            in_specs=[full(pltpu.SMEM)] + [full()] * (3 + len(restored)),
            out_specs=full(),
            **settings(12, 1),
        )(table, rank, t, slopes, *restored)
        operands = [found, weights, *columns, *gates]
        gate_values, increments = pl.pallas_call(
            functools.partial(final_kernel, tile_count, sites, picks, len(columns)),
            out_shape=[shape(gate_adjoint.shape, f32), shape(mixing.shape, f32)],
            in_specs=[full()] * len(operands),
            out_specs=[full(pltpu.HBM)] * 2,
            scratch_shapes=[
                pltpu.VMEM((gate_dev, len(group) * capacity), f32),
                picked,
                pltpu.SemaphoreType.DMA,
            ] + [pltpu.SemaphoreType.DMA((len(site),)) for site in sites],
            **settings(16, 2),
        )(*operands)
    return gate_values, increments


def solution(mesh):
    return jax.shard_map(
        per_device,
        mesh=mesh,
        in_specs=(
            P(None, "lev", "tile"),
            P("lev", "tile"),
            P("tile", None),
            P("tile", None, None),
            P("lev", "tile"),
        ),
        out_specs=(P("lev", "tile"), P(None, "lev", "tile")),
        check_vma=False,
    )
```
